512 devices in a mesh: section: 16 (over z_hi, y), dp: 4 (over x), tensor: 8 (over z_lo, core).
Axes of the slice: x: 4, y: 8, z: 8 (z_hi: 2, z_lo: 4; z = z_hi * 4 + z_lo), core: 2. Of those that a mesh axis runs over, the one named last changes fastest.
Arguments:
- sent_out: bfloat16 [16, 2, 768, 4096], P('section', None, 'dp', 'tensor'), may hold values from -6 to 6
- sent_back: bfloat16 [16, 2, 768, 4096], P('section', None, 'dp', 'tensor'), may hold values from -6 to 6
- sent_grad: bfloat16 [16, 2, 768, 4096], P('section', None, 'dp', 'tensor'), may hold values from -6 to 6
- lengths: int32 [16, 4], P('section', 'dp'), may hold values from 48 to 192
- weight: bfloat16 [16, 4096, 4096], P('section', 'dp', 'tensor'), may hold values from -0.09375 to 0.09375
Outputs:
- emitted: bfloat16 [16, 2, 768, 4096], P('section', None, 'dp', 'tensor')
- rebuilt: bfloat16 [16, 2, 768, 4096], P('section', None, 'dp', 'tensor')
- input_grad: bfloat16 [16, 2, 768, 4096], P('section', None, 'dp', 'tensor')
- weight_grad: bfloat16 [16, 4096, 4096], P('section', 'dp', 'tensor')
The draws below stay inside these ranges and needn't reach their ends.
All inputs are finite; a program needn't handle non-finite values.
Results may differ from the reference program's by a relative error of at most 0.0075.
Values may be sent and summed in bfloat16 or wider, within the bound.
No kernel may reach another device: no remote copies, remote signals or barrier semaphores. Data moves between devices by JAX's collectives and lax.ppermute only.
A program may use at most 64 MiB of HBM per device.

```python
import jax
import jax.numpy as jnp
from jax import lax

HALF = 4096
TOK = 192
SECTIONS = 16
REPLICAS = 4
ROWS = 768
N_TENSOR = 8


def set_ends(array, stream_key, low, top_value):
    dims = array.shape
    place = [jax.random.randint(jax.random.fold_in(stream_key, axis), (), 0, dims[axis]) for axis in range(len(dims))]
    array = array.at[tuple(place)].set(low)
    longest = dims.index(max(dims))
    place[longest] = (place[longest] + 1) % dims[longest]
    return array.at[tuple(place)].set(top_value)


def block_levels(key, shape, cuts, least, high):
    gain, own = 1.0, jax.random.fold_in(key, 6)
    for dim, shards_of in cuts:
        steps = jnp.exp(jax.random.uniform(jax.random.fold_in(own, dim), (shards_of,), jnp.float32, least / len(cuts), high / len(cuts)))
        gain = gain * jnp.repeat(steps, shape[dim] // shards_of).reshape([-1 if axis == dim else 1 for axis in range(len(shape))])
    return gain


def centred(rng, dims, deviation, most, pieces=(), kind=jnp.bfloat16):
    result = deviation * jax.random.normal(rng, dims, jnp.float32)
    if pieces:
        result = result * block_levels(rng, dims, pieces, -0.22, 0.18)
    return jnp.clip(result, -most, most).astype(kind)


def setup_inputs(seed: int = 0) -> dict:
    arg_keys = jax.random.split(jax.random.key(seed), 6)
    return {
        "sent_out": centred(arg_keys[0], (SECTIONS, 2, ROWS, HALF), 1.0, 6.0, ((0, 16), (2, 4), (3, 8))),
        "sent_back": centred(arg_keys[1], (SECTIONS, 2, ROWS, HALF), 1.0, 6.0, ((0, 16), (2, 4), (3, 8))),
        "sent_grad": centred(arg_keys[2], (SECTIONS, 2, ROWS, HALF), 1.0, 6.0, ((0, 16), (2, 4), (3, 8))),
        "lengths": set_ends(jax.random.randint(arg_keys[3], (SECTIONS, REPLICAS), TOK // 4, TOK + 1), jax.random.fold_in(arg_keys[3], 1), TOK // 4, TOK).astype(jnp.int32),
        "weight": centred(arg_keys[4], (SECTIONS, HALF, HALF), HALF ** -0.5, 0.09375, ((0, 16), (1, 4), (2, 8))),
    }


def across_rows(left, right):
    return lax.dot_general(left, right, (((0,), (0,)), ((), ())), preferred_element_type=jnp.float32)


def slope(hidden):
    sigma = jax.nn.sigmoid(hidden)
    return sigma * (1.0 + hidden * (1.0 - sigma))


def grouped_back(hidden, weights):
    count = hidden.shape[0]
    blocks = hidden.astype(jnp.float32).reshape(count, N_TENSOR, -1)
    tables = weights.astype(jnp.float32).reshape(weights.shape[0], N_TENSOR, -1)
    parts = jnp.einsum("rkc,jkc->krj", blocks, tables)
    return jnp.sum(parts.astype(jnp.bfloat16).astype(jnp.float32), axis=0)


def reference(sent_out, sent_back, sent_grad, lengths, weight):
    inbound = jnp.roll(sent_out, 1, axis=0)
    back = jnp.roll(sent_back, -1, axis=0)
    incoming = jnp.roll(sent_grad, -1, axis=0)
    total_rows = sent_out.shape[2]
    position = jnp.arange(total_rows, dtype=jnp.int32) % TOK
    replica = jnp.arange(total_rows, dtype=jnp.int32) // TOK
    zero = jnp.zeros((), jnp.bfloat16)
    emitted, rebuilt, input_grad, weight_grad = [], [], [], []
    for section_index in range(SECTIONS):
        matrix = weight[section_index]
        upper_in, lower_in = inbound[section_index, 0], inbound[section_index, 1]
        pre = jnp.dot(upper_in, matrix, preferred_element_type=jnp.float32)
        upper_out = (lower_in.astype(jnp.float32) + jax.nn.silu(pre)).astype(jnp.bfloat16)
        emitted.append(jnp.stack([upper_out, upper_in]))
        back_upper, back_lower = back[section_index, 0], back[section_index, 1]
        pre_held = jnp.dot(back_lower, matrix, preferred_element_type=jnp.float32)
        rebuilt_lower = (back_upper.astype(jnp.float32) - jax.nn.silu(pre_held)).astype(jnp.bfloat16)
        rebuilt.append(jnp.stack([back_lower, rebuilt_lower]))
        limit = lengths[section_index][replica]
        keep = (position < limit)[:, None]
        dupper = jnp.where(keep, incoming[section_index, 0], zero)
        dlower = jnp.where(keep, incoming[section_index, 1], zero)
        hidden = (dupper.astype(jnp.float32) * slope(pre_held)).astype(jnp.bfloat16)
        dupper_in = (dlower.astype(jnp.float32) + grouped_back(hidden, matrix)).astype(jnp.bfloat16)
        input_grad.append(jnp.stack([dupper_in, dupper]))
        weight_grad.append(across_rows(back_lower, hidden).astype(jnp.bfloat16))
    return (jnp.stack(emitted), jnp.stack(rebuilt), jnp.stack(input_grad), jnp.stack(weight_grad))
```

```python
import jax
import jax.numpy as jnp
from jax import lax
from jax.experimental import pallas as pl
from jax.experimental.pallas import tpu as pltpu
from jax.sharding import PartitionSpec as P


F32 = jnp.float32
BF16 = jnp.bfloat16


def shifted(block, axis, distance):
    devices = range(lax.axis_size(axis))
    route = [((i - distance) % len(devices), i) for i in devices]
    return lax.ppermute(block, axis, route)


def exchanged(block, flip):
    return lax.ppermute(block, "tensor", [(i, i ^ flip) for i in range(lax.axis_size("tensor"))])


def nn(left, right):
    return lax.dot_general(left, right, (((1,), (0,)), ((), ())), preferred_element_type=F32)


def nt(left, right):
    return lax.dot_general(left, right, (((1,), (1,)), ((), ())), preferred_element_type=F32)


def tn(left, right):
    return lax.dot_general(left, right, (((0,), (0,)), ((), ())), preferred_element_type=F32)


def places():
    along = lax.axis_index("tensor")
    return lax.axis_index("dp"), lax.div(along, 2), lax.rem(along, 2)


def shards(own, prev, nxt, far_lo, far_hi):
    half = own.shape[0] // 2
    return (
        (0, own[:half], own[half:]),
        (3, prev[:half], prev[half:]),
        (1, nxt[:half], nxt[half:]),
        (2, far_lo[...], far_hi[...]),
    )


def by_parity(core, mine, other):
    first = core == 0
    return jnp.where(first, mine, other), jnp.where(first, other, mine)


def slot(chip, k):
    e = lax.bitwise_xor(chip, k)
    return lax.rem(e, 2), lax.div(e, 2)


def picked(own_pair, near_pair, chip, k):
    which, at = slot(chip, k)
    return jnp.where(which == 0, own_pair[at], near_pair[at])


def project(mine, other, parts):
    place, chip, core = places()
    total = None
    for distance, low, high in parts:
        k = lax.rem(place + distance, 4)
        even, odd = by_parity(core, picked(*mine, chip, k), picked(*other, chip, k))
        term = nn(even, low) + nn(odd, high)
        total = term if total is None else total + term
    return total


def held_kernel(
    length, mine_a, mine_b, other_a, other_b, own, prev, nxt, far_lo, far_hi, grad, pre_out, keep_out, send_out, dp_out
):
    place, chip, core = places()
    parts = shards(own, prev, nxt, far_lo, far_hi)
    pre = project((mine_a, mine_b), (other_a, other_b), parts)
    pre_out[...] = pre
    sigma = jax.nn.sigmoid(pre)
    live = lax.broadcasted_iota(jnp.int32, pre.shape, 0) < length[0, 0]
    dupper = jnp.where(live, grad[0, 0].astype(F32), 0.0)
    hidden = (dupper * (sigma * (1.0 + pre * (1.0 - sigma)))).astype(BF16)
    for k in range(4):
        dp_out[k, 0] = picked(mine_a, mine_b, chip, k)
        dp_out[k, 1] = hidden
    for distance, low, high in parts:
        k = lax.rem(place + distance, 4)
        even = nt(hidden, low).astype(BF16)
        odd = nt(hidden, high).astype(BF16)
        which, at = slot(chip, k)
        keep, send = by_parity(core, even, odd)
        keep_out[which, at] = keep
        send_out[which, at] = send


def new_kernel(mine_a, mine_b, other_a, other_b, own, prev, nxt, far_lo, far_hi, inbound, out):
    pre = project((mine_a, mine_b), (other_a, other_b), shards(own, prev, nxt, far_lo, far_hi))
    out[0, 0] = (inbound[0, 1].astype(F32) + pre * jax.nn.sigmoid(pre)).astype(BF16)
    out[0, 1] = inbound[0, 0]


def rebuilt_kernel(pre, back, out):
    t = pre[...]
    out[0, 0] = back[0, 1]
    out[0, 1] = (back[0, 0].astype(F32) - t * jax.nn.sigmoid(t)).astype(BF16)


def grad_kernel(exchange, other, out):
    _, _, core = places()
    half = out.shape[1] // 2
    hidden = exchange[:, 1].reshape(-1, exchange.shape[-1])
    even, odd = by_parity(core, exchange[:, 0], other[...])
    out[0, :half] = tn(even.reshape(-1, half), hidden).astype(BF16)
    out[0, half:] = tn(odd.reshape(-1, half), hidden).astype(BF16)


def near_kernel(keep, received, out):
    out[...] = (keep[1].astype(F32) + received[1].astype(F32)).astype(BF16)


def far_kernel(keep, received, near, out):
    out[...] = (keep[0, 1].astype(F32) + received[0, 1].astype(F32) + near[1].astype(F32)).astype(BF16)


def last_kernel(length, keep, received, near, far, grad, out):
    live = lax.broadcasted_iota(jnp.int32, far.shape, 0) < length[0, 0]
    through = keep[0, 0].astype(F32) + received[0, 0].astype(F32) + near[0].astype(F32) + far[...].astype(F32)
    out[0, 0] = (jnp.where(live, grad[0, 1].astype(F32), 0.0) + through).astype(BF16)
    out[0, 1] = jnp.where(live, grad[0, 0].astype(F32), 0.0).astype(BF16)


def run(kernel, outs, args, flops=0, scalars=0, mib=8):
    vmem = pl.BlockSpec(memory_space=pltpu.VMEM)
    smem = pl.BlockSpec(memory_space=pltpu.SMEM)
    moved = sum(a.size * a.dtype.itemsize for a in args)
    return pl.pallas_call(
        kernel,
        out_shape=outs,
        in_specs=[smem] * scalars + [vmem] * (len(args) - scalars),
        out_specs=jax.tree.map(lambda _: vmem, outs),
        cost_estimate=pl.CostEstimate(flops=flops, transcendentals=0, bytes_accessed=moved),
        compiler_params=pltpu.CompilerParams(vmem_limit_bytes=mib * 2**20),
    )(*args)


def gathered(block):
    far = exchanged(block, 4)
    own_pair = jnp.stack([block, far])
    near_pair = exchanged(own_pair, 2)
    other_own = exchanged(own_pair, 1)
    other_near = exchanged(near_pair, 1)
    return own_pair, near_pair, other_own, other_near


def local(sent_out, sent_back, sent_grad, lengths, weight):
    tokens, width = sent_out.shape[2:]
    own = weight[0]
    depth = own.shape[0]
    half = depth // 2
    shape = jax.ShapeDtypeStruct
    pair = shape((1, 2, tokens, width), BF16)
    product = 2 * tokens * width * 4 * depth

    prev = shifted(own, "dp", 1)
    nxt = shifted(own, "dp", -1)
    back = shifted(sent_back, "section", -1)
    inbound = shifted(sent_out, "section", 1)
    grad = shifted(sent_grad, "section", -1)
    far_lo = shifted(prev[:half], "dp", 1)
    far_hi = shifted(nxt[half:], "dp", -1)
    weights = (own, prev, nxt, far_lo, far_hi)
    held = gathered(back[0, 1])
    new = gathered(inbound[0, 0])

    terms = shape((2, 2, tokens, width), BF16)
    pre_held, keep, send, share = run(
        held_kernel,
        (shape((tokens, width), F32), terms, terms, shape((4, 2, tokens, width), BF16)),
        (lengths, *held, *weights, grad),
        flops=2 * product,
        scalars=1,
        mib=20,
    )
    received = exchanged(send, 1)
    exchange = lax.all_to_all(share, "dp", 0, 0, tiled=True)
    near_sum = run(near_kernel, shape((2, tokens, width), BF16), (keep, received))
    near = exchanged(near_sum, 2)
    emitted = run(new_kernel, pair, (*new, *weights, inbound), flops=product, mib=16)
    far_sum = run(far_kernel, shape((tokens, width), BF16), (keep, received, near))
    far = exchanged(far_sum, 4)
    rebuilt = run(rebuilt_kernel, pair, (pre_held, back), flops=tokens * width)
    other = exchanged(exchange[:, 0], 1)
    weight_grad = run(grad_kernel, shape(weight.shape, BF16), (exchange, other), flops=product, mib=16)
    input_grad = run(last_kernel, pair, (lengths, keep, received, near, far, grad), scalars=1)
    return emitted, rebuilt, input_grad, weight_grad


def solution(mesh):
    act = P("section", None, "dp", "tensor")
    mat = P("section", "dp", "tensor")
    return jax.shard_map(
        local,
        mesh=mesh,
        in_specs=(act, act, act, P("section", "dp"), mat),
        out_specs=(act, act, act, mat),
        check_vma=False,
    )
```

```python
import jax
import jax.numpy as jnp
from jax import lax
from jax.experimental import pallas as pl
from jax.experimental.pallas import tpu as pltpu
from jax.sharding import PartitionSpec as P


F32 = jnp.float32
BF16 = jnp.bfloat16


def shifted(block, axis, distance):
    devices = range(lax.axis_size(axis))
    route = [((i - distance) % len(devices), i) for i in devices]
    return lax.ppermute(block, axis, route)


def exchanged(block, flip):
    return lax.ppermute(block, "tensor", [(i, i ^ flip) for i in range(lax.axis_size("tensor"))])


def nn(left, right):
    return lax.dot_general(left, right, (((1,), (0,)), ((), ())), preferred_element_type=F32)


def nt(left, right):
    return lax.dot_general(left, right, (((1,), (1,)), ((), ())), preferred_element_type=F32)


def tn(left, right):
    return lax.dot_general(left, right, (((0,), (0,)), ((), ())), preferred_element_type=F32)


def places():
    along = lax.axis_index("tensor")
    return lax.axis_index("dp"), lax.div(along, 2), lax.rem(along, 2)


def shards(own, prev, nxt, far_lo, far_hi):
    half = own.shape[0] // 2
    return (
        (0, own[:half], own[half:]),
        (3, prev[:half], prev[half:]),
        (1, nxt[:half], nxt[half:]),
        (2, far_lo[...], far_hi[...]),
    )


def by_parity(core, mine, other):
    first = core == 0
    return jnp.where(first, mine, other), jnp.where(first, other, mine)


def slot(chip, k):
    e = lax.bitwise_xor(chip, k)
    return lax.rem(e, 2), lax.div(e, 2)


def picked(own_pair, near_pair, chip, k):
    which, at = slot(chip, k)
    return jnp.where(which == 0, own_pair[at], near_pair[at])


def project(mine, other, parts):
    place, chip, core = places()
    total = None
    for distance, low, high in parts:
        k = lax.rem(place + distance, 4)
        even, odd = by_parity(core, picked(*mine, chip, k), picked(*other, chip, k))
        term = nn(even, low) + nn(odd, high)
        total = term if total is None else total + term
    return total


def held_kernel(
    length, mine_a, mine_b, other_a, other_b, own, prev, nxt, far_lo, far_hi, grad, keep_out, send_out, own_out, dp_1, dp_2, dp_3, pre_out
):
    place, chip, core = places()
    parts = shards(own, prev, nxt, far_lo, far_hi)
    pre = project((mine_a, mine_b), (other_a, other_b), parts)
    sigma = jax.nn.sigmoid(pre)
    pre_out[...] = pre
    live = lax.broadcasted_iota(jnp.int32, pre.shape, 0) < length[0, 0]
    dupper = jnp.where(live, grad[...].astype(F32), 0.0)
    hidden = (dupper * (sigma * (1.0 + pre * (1.0 - sigma)))).astype(BF16)
    own_out[0] = picked(mine_a, mine_b, chip, place)
    own_out[1] = picked(other_a, other_b, chip, place)
    own_out[2] = hidden
    for distance, out in ((1, dp_1), (2, dp_2), (3, dp_3)):
        out[0] = picked(mine_a, mine_b, chip, lax.rem(place + distance, 4))
        out[1] = hidden
    for distance, low, high in parts:
        k = lax.rem(place + distance, 4)
        even = nt(hidden, low).astype(BF16)
        odd = nt(hidden, high).astype(BF16)
        which, at = slot(chip, k)
        keep, send = by_parity(core, even, odd)
        keep_out[which, at] = keep
        send_out[which, at] = send


def new_kernel(mine_a, mine_b, other_a, other_b, own, prev, nxt, far_lo, far_hi, inbound, out):
    pre = project((mine_a, mine_b), (other_a, other_b), shards(own, prev, nxt, far_lo, far_hi))
    out[0, 0] = (inbound[0, 1].astype(F32) + pre * jax.nn.sigmoid(pre)).astype(BF16)
    out[0, 1] = inbound[0, 0]


def split_kernel(back, grad, held_out, grad_out, late_out):
    held_out[...] = back[0, 1]
    grad_out[...] = grad[0, 0]
    late_out[0] = back[0, 0]
    late_out[1] = grad[0, 1]


def rebuilt_kernel(pre, lower, late, wrap, out):
    t = pre[...]
    out[0, 0] = lower[...]
    out[0, 1] = ((late[0] + wrap[0]).astype(F32) - t * jax.nn.sigmoid(t)).astype(BF16)


def grad_kernel(own, dp_1, dp_2, dp_3, swapped, out):
    _, _, core = places()
    half = out.shape[1] // 2
    hidden = jnp.concatenate([own[2], dp_1[1], dp_2[1], dp_3[1]])
    mine = jnp.concatenate([own[0], dp_1[0], dp_2[0], dp_3[0]])
    other = jnp.concatenate([own[1], swapped[0], swapped[1], swapped[2]])
    even, odd = by_parity(core, mine, other)
    out[0, :half] = tn(even, hidden).astype(BF16)
    out[0, half:] = tn(odd, hidden).astype(BF16)


def share_kernel(dp_1, dp_2, dp_3, out):
    out[0] = dp_1[0]
    out[1] = dp_2[0]
    out[2] = dp_3[0]


def stack_kernel(first, second, out):
    out[0] = first[...]
    out[1] = second[...]


def near_kernel(keep, received, out):
    out[...] = (keep[1].astype(F32) + received[1].astype(F32)).astype(BF16)


def far_kernel(keep, received, near, out):
    out[...] = (keep[0, 1].astype(F32) + received[0, 1].astype(F32) + near[1].astype(F32)).astype(BF16)


def last_kernel(length, keep, received, near, far, upper, late, wrap, out):
    live = lax.broadcasted_iota(jnp.int32, far.shape, 0) < length[0, 0]
    through = keep[0, 0].astype(F32) + received[0, 0].astype(F32) + near[0].astype(F32) + far[...].astype(F32)
    out[0, 0] = (jnp.where(live, (late[1] + wrap[1]).astype(F32), 0.0) + through).astype(BF16)
    out[0, 1] = jnp.where(live, upper[...].astype(F32), 0.0).astype(BF16)


def run(kernel, outs, args, flops=0, scalars=0, mib=8):
    vmem = pl.BlockSpec(memory_space=pltpu.VMEM)
    smem = pl.BlockSpec(memory_space=pltpu.SMEM)
    moved = sum(a.size * a.dtype.itemsize for a in args)
    return pl.pallas_call(
        kernel,
        out_shape=outs,
        in_specs=[smem if n < scalars else vmem for n in range(len(args))],
        out_specs=jax.tree.map(lambda _: vmem, outs),
        cost_estimate=pl.CostEstimate(flops=flops, transcendentals=0, bytes_accessed=moved),
        compiler_params=pltpu.CompilerParams(vmem_limit_bytes=mib * 2**20),
    )(*args)


def gathered(block):
    far = exchanged(block, 4)
    own_pair = run(stack_kernel, jax.ShapeDtypeStruct((2, *block.shape), BF16), (block, far))
    near_pair = exchanged(own_pair, 2)
    other_own = exchanged(own_pair, 1)
    other_near = exchanged(near_pair, 1)
    return own_pair, near_pair, other_own, other_near


def local(sent_out, sent_back, sent_grad, lengths, weight):
    tokens, width = sent_out.shape[2:]
    own = weight[0]
    depth = own.shape[0]
    half = depth // 2
    shape = jax.ShapeDtypeStruct
    pair = shape((1, 2, tokens, width), BF16)
    block = shape((tokens, width), BF16)
    two = shape((2, tokens, width), BF16)
    three = shape((3, tokens, width), BF16)
    product = 2 * tokens * width * 4 * depth

    prev = shifted(own, "dp", 1)
    nxt = shifted(own, "dp", -1)
    held_out, grad_out, late_out = run(split_kernel, (block, block, two), (sent_back, sent_grad))
    back_lower = shifted(held_out, "section", -1)
    inbound = shifted(sent_out, "section", 1)
    grad_upper = shifted(grad_out, "section", -1)
    count = lax.axis_size("section")
    rank = count // 2
    across = lax.ppermute(late_out, "section", [(0, rank + 1), (rank, 1)])
    late = lax.ppermute(late_out, "section", [(i, i - 1) for i in range(count) if i % rank])
    late_wrap = lax.ppermute(across, "section", [(rank + 1, count - 1), (1, rank - 1)])
    far_lo = shifted(prev[:half], "dp", 1)
    far_hi = shifted(nxt[half:], "dp", -1)
    weights = (own, prev, nxt, far_lo, far_hi)
    upper_in = inbound[0, 0]
    held = gathered(back_lower)
    new = gathered(upper_in)

    terms = shape((2, 2, tokens, width), BF16)
    keep, send, own_share, *to_dp, pre_held = run(
        held_kernel,
        (terms, terms, three, two, two, two, shape((tokens, width), F32)),
        (lengths, *held, *weights, grad_upper),
        flops=2 * product,
        scalars=1,
        mib=20,
    )
    received = exchanged(send, 1)
    from_dp = []
    for distance in (1, 2, 3):
        from_dp.append(shifted(to_dp[distance - 1], "dp", distance))
    near_sum = run(near_kernel, shape((2, tokens, width), BF16), (keep, received))
    near = exchanged(near_sum, 2)
    emitted = run(new_kernel, pair, (*new, *weights, inbound), flops=product, mib=16)
    far_sum = run(far_kernel, shape((tokens, width), BF16), (keep, received, near))
    far = exchanged(far_sum, 4)
    rebuilt = run(rebuilt_kernel, pair, (pre_held, back_lower, late, late_wrap), flops=tokens * width)
    shares = run(share_kernel, three, from_dp)
    other = exchanged(shares, 1)
    weight_grad = run(grad_kernel, shape(weight.shape, BF16), (own_share, *from_dp, other), flops=product, mib=16)
    input_grad = run(last_kernel, pair, (lengths, keep, received, near, far, grad_upper, late, late_wrap), scalars=1)
    return emitted, rebuilt, input_grad, weight_grad


def solution(mesh):
    act = P("section", None, "dp", "tensor")
    mat = P("section", "dp", "tensor")
    return jax.shard_map(
        local,
        mesh=mesh,
        in_specs=(act, act, act, P("section", "dp"), mat),
        out_specs=(act, act, act, mat),
        check_vma=False,
    )
```

```python
import jax
import jax.numpy as jnp
from jax import lax
from jax.experimental import pallas as pl
from jax.experimental.pallas import tpu as pltpu
from jax.sharding import PartitionSpec as P


F32 = jnp.float32
BF16 = jnp.bfloat16


def shifted(block, axis, distance):
    devices = range(lax.axis_size(axis))
    route = [((i - distance) % len(devices), i) for i in devices]
    return lax.ppermute(block, axis, route)


def exchanged(block, flip):
    return lax.ppermute(block, "tensor", [(i, i ^ flip) for i in range(lax.axis_size("tensor"))])


def nn(left, right):
    return lax.dot_general(left, right, (((1,), (0,)), ((), ())), preferred_element_type=F32)


def nt(left, right):
    return lax.dot_general(left, right, (((1,), (1,)), ((), ())), preferred_element_type=F32)


def tn(left, right):
    return lax.dot_general(left, right, (((0,), (0,)), ((), ())), preferred_element_type=F32)


def places():
    along = lax.axis_index("tensor")
    return lax.axis_index("dp"), lax.div(along, 2), lax.rem(along, 2)


def shards(own, prev, nxt, far_lo, far_hi):
    half = own.shape[0] // 2
    return (
        (0, own[:half], own[half:]),
        (3, prev[:half], prev[half:]),
        (1, nxt[:half], nxt[half:]),
        (2, far_lo[...], far_hi[...]),
    )


def by_parity(core, mine, other):
    first = core == 0
    return jnp.where(first, mine, other), jnp.where(first, other, mine)


def slot(chip, k):
    e = lax.bitwise_xor(chip, k)
    return lax.rem(e, 2), lax.div(e, 2)


def picked(own_pair, near_pair, chip, k):
    which, at = slot(chip, k)
    return jnp.where(which == 0, own_pair[at], near_pair[at])


def project(mine, other, parts):
    place, chip, core = places()
    total = None
    for distance, low, high in parts:
        k = lax.rem(place + distance, 4)
        even, odd = by_parity(core, picked(*mine, chip, k), picked(*other, chip, k))
        term = nn(even, low) + nn(odd, high)
        total = term if total is None else total + term
    return total


def held_kernel(
    length, mine_a, mine_b, other_a, other_b, own, prev, nxt, far_lo, far_hi, grad, keep_out, send_out, own_out, dp_1, dp_2, dp_3, pre_out
):
    place, chip, core = places()
    parts = shards(own, prev, nxt, far_lo, far_hi)
    pre = project((mine_a, mine_b), (other_a, other_b), parts)
    sigma = jax.nn.sigmoid(pre)
    pre_out[...] = pre
    live = lax.broadcasted_iota(jnp.int32, pre.shape, 0) < length[0, 0]
    dupper = jnp.where(live, grad[...].astype(F32), 0.0)
    hidden = (dupper * (sigma * (1.0 + pre * (1.0 - sigma)))).astype(BF16)
    own_out[0] = picked(mine_a, mine_b, chip, place)
    own_out[1] = picked(other_a, other_b, chip, place)
    own_out[2] = hidden
    for distance, out in ((1, dp_1), (2, dp_2), (3, dp_3)):
        out[0] = picked(mine_a, mine_b, chip, lax.rem(place + distance, 4))
        out[1] = hidden
    for distance, low, high in parts:
        k = lax.rem(place + distance, 4)
        even = nt(hidden, low).astype(BF16)
        odd = nt(hidden, high).astype(BF16)
        which, at = slot(chip, k)
        keep, send = by_parity(core, even, odd)
        keep_out[which, at] = keep
        send_out[which, at] = send


def new_kernel(mine_a, mine_b, other_a, other_b, own, prev, nxt, far_lo, far_hi, upper, lower, out):
    pre = project((mine_a, mine_b), (other_a, other_b), shards(own, prev, nxt, far_lo, far_hi))
    out[0, 0] = (lower[...].astype(F32) + pre * jax.nn.sigmoid(pre)).astype(BF16)
    out[0, 1] = upper[...]


def split_kernel(back, grad, held_out, grad_out, late_out):
    held_out[...] = back[0, 1]
    grad_out[...] = grad[0, 0]
    late_out[0] = back[0, 0]
    late_out[1] = grad[0, 1]


def rebuilt_kernel(pre, lower, late, wrap, out):
    t = pre[...]
    out[0, 0] = lower[...]
    out[0, 1] = ((late[0] + wrap[0]).astype(F32) - t * jax.nn.sigmoid(t)).astype(BF16)


def grad_kernel(own, dp_1, dp_2, dp_3, swapped, out):
    _, _, core = places()
    half = out.shape[1] // 2
    hidden = jnp.concatenate([own[2], dp_1[1], dp_2[1], dp_3[1]])
    mine = jnp.concatenate([own[0], dp_1[0], dp_2[0], dp_3[0]])
    other = jnp.concatenate([own[1], swapped[0], swapped[1], swapped[2]])
    even, odd = by_parity(core, mine, other)
    out[0, :half] = tn(even, hidden).astype(BF16)
    out[0, half:] = tn(odd, hidden).astype(BF16)


def share_kernel(dp_1, dp_2, dp_3, out):
    out[0] = dp_1[0]
    out[1] = dp_2[0]
    out[2] = dp_3[0]


def stack_kernel(first, second, out):
    out[0] = first[...]
    out[1] = second[...]


def near_kernel(keep, received, out):
    out[...] = (keep[1].astype(F32) + received[1].astype(F32)).astype(BF16)


def far_kernel(keep, received, near, out):
    out[...] = (keep[0, 1].astype(F32) + received[0, 1].astype(F32) + near[1].astype(F32)).astype(BF16)


def last_kernel(length, keep, received, near, far, upper, late, wrap, out):
    live = lax.broadcasted_iota(jnp.int32, far.shape, 0) < length[0, 0]
    through = keep[0, 0].astype(F32) + received[0, 0].astype(F32) + near[0].astype(F32) + far[...].astype(F32)
    out[0, 0] = (jnp.where(live, (late[1] + wrap[1]).astype(F32), 0.0) + through).astype(BF16)
    out[0, 1] = jnp.where(live, upper[...].astype(F32), 0.0).astype(BF16)


def run(kernel, outs, args, flops=0, scalars=0, mib=8):
    vmem = pl.BlockSpec(memory_space=pltpu.VMEM)
    smem = pl.BlockSpec(memory_space=pltpu.SMEM)
    moved = sum(a.size * a.dtype.itemsize for a in args)
    return pl.pallas_call(
        kernel,
        out_shape=outs,
        in_specs=[smem if n < scalars else vmem for n in range(len(args))],
        out_specs=jax.tree.map(lambda _: vmem, outs),
        cost_estimate=pl.CostEstimate(flops=flops, transcendentals=0, bytes_accessed=moved),
        compiler_params=pltpu.CompilerParams(vmem_limit_bytes=mib * 2**20),
    )(*args)


def gathered(block):
    far = exchanged(block, 4)
    own_pair = run(stack_kernel, jax.ShapeDtypeStruct((2, *block.shape), BF16), (block, far))
    near_pair = exchanged(own_pair, 2)
    other_own = exchanged(own_pair, 1)
    other_near = exchanged(near_pair, 1)
    return own_pair, near_pair, other_own, other_near


def local(sent_out, sent_back, sent_grad, lengths, weight):
    tokens, width = sent_out.shape[2:]
    own = weight[0]
    depth = own.shape[0]
    half = depth // 2
    shape = jax.ShapeDtypeStruct
    pair = shape((1, 2, tokens, width), BF16)
    block = shape((tokens, width), BF16)
    two = shape((2, tokens, width), BF16)
    three = shape((3, tokens, width), BF16)
    product = 2 * tokens * width * 4 * depth

    prev = shifted(own, "dp", 1)
    nxt = shifted(own, "dp", -1)
    held_out, grad_out, late_out = run(split_kernel, (block, block, two), (sent_back, sent_grad))
    back_lower = shifted(held_out, "section", -1)
    upper_in = shifted(sent_out[0, 0], "section", 1)
    lower_in = shifted(sent_out[0, 1], "section", 1)
    grad_upper = shifted(grad_out, "section", -1)
    count = lax.axis_size("section")
    rank = count // 2
    across = lax.ppermute(late_out, "section", [(0, rank + 1), (rank, 1)])
    late = lax.ppermute(late_out, "section", [(i, i - 1) for i in range(count) if i % rank])
    late_wrap = lax.ppermute(across, "section", [(rank + 1, count - 1), (1, rank - 1)])
    far_lo = shifted(prev[:half], "dp", 1)
    far_hi = shifted(nxt[half:], "dp", -1)
    weights = (own, prev, nxt, far_lo, far_hi)
    held = gathered(back_lower)
    new = gathered(upper_in)

    terms = shape((2, 2, tokens, width), BF16)
    keep, send, own_share, *to_dp, pre_held = run(
        held_kernel,
        (terms, terms, three, two, two, two, shape((tokens, width), F32)),
        (lengths, *held, *weights, grad_upper),
        flops=2 * product,
        scalars=1,
        mib=20,
    )
    received = exchanged(send, 1)
    from_dp = []
    for distance in (1, 2, 3):
        from_dp.append(shifted(to_dp[distance - 1], "dp", distance))
    near_sum = run(near_kernel, shape((2, tokens, width), BF16), (keep, received))
    near = exchanged(near_sum, 2)
    emitted = run(new_kernel, pair, (*new, *weights, upper_in, lower_in), flops=product, mib=16)
    far_sum = run(far_kernel, shape((tokens, width), BF16), (keep, received, near))
    far = exchanged(far_sum, 4)
    rebuilt = run(rebuilt_kernel, pair, (pre_held, back_lower, late, late_wrap), flops=tokens * width)
    shares = run(share_kernel, three, from_dp)
    other = exchanged(shares, 1)
    weight_grad = run(grad_kernel, shape(weight.shape, BF16), (own_share, *from_dp, other), flops=product, mib=16)
    input_grad = run(last_kernel, pair, (lengths, keep, received, near, far, grad_upper, late, late_wrap), scalars=1)
    return emitted, rebuilt, input_grad, weight_grad


def solution(mesh):
    act = P("section", None, "dp", "tensor")
    mat = P("section", "dp", "tensor")
    return jax.shard_map(
        local,
        mesh=mesh,
        in_specs=(act, act, act, P("section", "dp"), mat),
        out_specs=(act, act, act, mat),
        check_vma=False,
    )
```
